32 devices in a mesh: grp: 2 (over x), row: 8 (over z, y), col: 2 (over core).
Axes of the slice: x: 2, y: 2, z: 4, core: 2. Of those that a mesh axis runs over, the one named last changes fastest.
Arguments:
- density: bfloat16 [1024, 32, 128], P(('grp', 'row', 'col')), parts along dimension 0, may hold values from -6 to 6
- leaf_target: int32 [1024], P(('grp', 'row', 'col')), parts along dimension 0, may hold values from 0 to 511, as said below
- geometry: float32 [6, 131072], P(None, ('grp', 'row', 'col')), parts along dimension 1, may hold values from -6 to 6
- near_list: int32 [1024, 16], P(('grp', 'row', 'col')), parts along dimension 0, may hold values from -1 to 511, as said below
- far_list: int32 [1024, 16], P(('grp', 'row', 'col')), parts along dimension 0, may hold values from -1 to 511, as said below
- node_list: int32 [128, 32], P(('grp', 'row', 'col')), parts along dimension 0, may hold values from -1 to 63, as said below
- basis_in: bfloat16 [1024, 64, 128], P(('grp', 'row', 'col')), parts along dimension 0, may hold values from -0.5 to 0.5
- basis_out: bfloat16 [1024, 64, 128], P(('grp', 'row', 'col')), parts along dimension 0, may hold values from -0.75 to 0.75
- transfer: bfloat16 [128, 64, 512], P(('grp', 'row', 'col')), parts along dimension 0, may hold values from -0.25 to 0.25
- node_points: float32 [3, 8192], P(None, 'grp'), parts along dimension 1, may hold values from -6 to 6
Outputs:
- potential: bfloat16 [1024, 32, 128], P(('grp', 'row', 'col')), parts along dimension 0
The draws below stay inside these ranges and needn't reach their ends.
There are 2 independent parts, one for each index of `grp`. The reference program is written for one: setup_inputs(seed, part) draws one part's arguments, and reference() takes and returns one part's arrays. A program takes and returns all parts, laid end to end along the dimension named above; each array names one. Nothing has to cross between parts.
Inputs may be any that keep to these rules, and one draw needn't show every extreme that they name: `leaf_target`: A permutation of the tree positions; of the 32 slab leaves of one device, exactly 2 go to the block of 32 tree positions of each device. `near_list`: row t holds t in slot 0; every other slot holds either -1 or a leaf other than t within 16 of t, the leaves of a row distinct; a -1 may stand in any slot after slot 0, also between leaves. `far_list`: every slot of row t holds either -1 or a leaf within 16 of t that is neither t nor in row t of near_list, the leaves of a row distinct; a -1 may stand in any slot, also between leaves. `node_list`: row p holds distinct nodes that differ from p by more than 2, then -1 in the unused slots.
All inputs are finite; a program needn't handle non-finite values.
Results may differ from the reference program's by a relative error of at most 0.0053.
Values may be sent and summed in bfloat16 or wider, within the bound.
A program may use at most 64 MiB of HBM per device.

```python
import math
import jax
import jax.numpy as jnp
from jax import lax

LEAF = 128
RANK = 64
NRHS = 32
CHILD = 8
REACH = 16
NEAR = 16
FAR = 16
FAR_NODE = 32
LEAF_DEV = 32
LEAVES = 512
PANELS = 65536
NODES = 64


def draw_leaf_target(key, part):
    shards = LEAVES // LEAF_DEV
    per_peer = LEAF_DEV // shards
    first_key, second_key = jax.random.split(jax.random.fold_in(key, 11))
    sender_order = jax.vmap(lambda item: jax.random.permutation(item, LEAF_DEV))(jax.random.split(first_key, shards))
    receiver_order = jax.vmap(lambda item: jax.random.permutation(item, LEAF_DEV))(jax.random.split(second_key, shards))
    sender_ids = jnp.arange(shards, dtype=jnp.int32)[:, None, None]
    receiver_ids = jnp.arange(shards, dtype=jnp.int32)[None, :, None]
    slab_pos = sender_ids * LEAF_DEV + sender_order.reshape(shards, shards, per_peer).astype(jnp.int32)
    tree_pos = receiver_ids * LEAF_DEV + receiver_order.reshape(shards, shards, per_peer).transpose(1, 0, 2).astype(jnp.int32)
    return jnp.zeros((LEAVES,), jnp.int32).at[slab_pos.reshape(-1)].set(tree_pos.reshape(-1))


def leaf_lists(key):
    first_key, second_key, third_key = jax.random.split(jax.random.fold_in(key, 5), 3)
    offsets = jnp.concatenate([jnp.arange(-REACH, 0), jnp.arange(1, REACH + 1)]).astype(jnp.int32)
    order = jax.vmap(lambda item: jax.random.permutation(item, 2 * REACH))(jax.random.split(first_key, LEAVES))
    chosen = offsets[order]
    target = jnp.arange(LEAVES, dtype=jnp.int32)[:, None]
    source = target + chosen
    inside = (source >= 0) & (source < LEAVES)
    near_live = jax.random.randint(second_key, (LEAVES, 1), NEAR // 4, NEAR)
    far_live = jax.random.randint(third_key, (LEAVES, 1), FAR // 2, FAR + 1)
    near_keep = inside[:, :NEAR - 1] & (jnp.arange(NEAR - 1)[None, :] < near_live)
    near_rows = jnp.concatenate([target, jnp.where(near_keep, source[:, :NEAR - 1], -1)], axis=1)
    far_keep = inside[:, NEAR - 1:NEAR - 1 + FAR] & (jnp.arange(FAR)[None, :] < far_live)
    far_rows = jnp.where(far_keep, source[:, NEAR - 1:NEAR - 1 + FAR], -1)
    return (near_rows.astype(jnp.int32), far_rows.astype(jnp.int32))


def draw_near_list(key, part):
    return leaf_lists(key)[0]


def draw_far_list(key, part):
    return leaf_lists(key)[1]


def draw_node_list(key, part):
    first_key, second_key = jax.random.split(jax.random.fold_in(key, 9))
    order = jax.vmap(lambda item: jax.random.permutation(item, NODES))(jax.random.split(first_key, NODES)).astype(jnp.int32)
    owner = jnp.arange(NODES, dtype=jnp.int32)[:, None]
    closeby = (jnp.abs(order - owner) <= 2).astype(jnp.int32)
    places = jnp.argsort(closeby, axis=1, stable=True)[:, :FAR_NODE]
    picked = jnp.take_along_axis(order, places, axis=1)
    live_count = jax.random.randint(second_key, (NODES, 1), FAR_NODE // 2, FAR_NODE + 1)
    return jnp.where(jnp.arange(FAR_NODE)[None, :] < live_count, picked, -1).astype(jnp.int32)


def steps_of(stream_key, shape, cuts, low, largest):
    loudness, own = 1.0, jax.random.fold_in(stream_key, 6)
    for dim, shards_of in cuts:
        draws = jnp.exp(jax.random.uniform(jax.random.fold_in(own, dim), (shards_of,), jnp.float32, low / len(cuts), largest / len(cuts)))
        loudness = loudness * jnp.repeat(draws, shape[dim] // shards_of).reshape([-1 if axis == dim else 1 for axis in range(len(shape))])
    return loudness


def normal_values(own_key, shape, width, limit, cuts=(), kind=jnp.bfloat16):
    level = steps_of(own_key, shape, cuts, -0.22, 0.18) if cuts else 1.0
    result = jax.random.normal(own_key, shape, jnp.float32) * width * level
    return jnp.minimum(jnp.maximum(result, -limit), limit).astype(kind)


def setup_inputs(seed: int = 0, part: int = 0) -> dict:
    arg_keys = jax.random.split(jax.random.key(seed), 11)
    part_keys = jax.random.split(jax.random.fold_in(arg_keys[10], part), 11)
    density = normal_values(part_keys[0], (LEAVES, NRHS, LEAF), 1.0, 6.0, ((0, 16),))
    leaf_target = draw_leaf_target(jax.random.fold_in(jax.random.fold_in(arg_keys[10], part), 71), part)
    geometry = normal_values(part_keys[2], (6, PANELS), 1.0, 6.0, ((1, 16),), jnp.float32)
    near_list = draw_near_list(jax.random.fold_in(jax.random.fold_in(arg_keys[10], part), 71), part)
    far_list = draw_far_list(jax.random.fold_in(jax.random.fold_in(arg_keys[10], part), 71), part)
    node_list = draw_node_list(jax.random.fold_in(jax.random.fold_in(arg_keys[10], part), 71), part)
    basis_in = normal_values(part_keys[6], (LEAVES, RANK, LEAF), LEAF ** -0.5, 0.5, ((0, 16),))
    basis_out = normal_values(part_keys[7], (LEAVES, RANK, LEAF), RANK ** -0.5, 0.75, ((0, 16),))
    transfer = normal_values(part_keys[8], (NODES, RANK, CHILD * RANK), (CHILD * RANK) ** -0.5, 0.25, ((0, 16),))
    node_points = normal_values(part_keys[9], (3, NODES * RANK), 1.0, 6.0, (), jnp.float32)
    return {"density": density, "leaf_target": leaf_target, "geometry": geometry, "near_list": near_list, "far_list": far_list, "node_list": node_list, "basis_in": basis_in, "basis_out": basis_out, "transfer": transfer, "node_points": node_points}


smoothing = 0.1
inv_four_pi = 0.25 / math.pi

def coupling(targets, sources):
    spread = targets - sources
    return inv_four_pi / jnp.sqrt(lax.optimization_barrier(jnp.sum(spread * spread, axis=0)) + smoothing * smoothing)

def double_layer(targets, sources, normals):
    spread = targets - sources
    distance = lax.optimization_barrier(jnp.sum(spread * spread, axis=0)) + smoothing * smoothing
    return inv_four_pi * lax.optimization_barrier(jnp.sum(normals * spread, axis=0)) / (distance * jnp.sqrt(distance))

def reference(density, leaf_target, geometry, near_list, far_list, node_list, basis_in, basis_out, transfer, node_points):
    source_rows = jnp.argsort(leaf_target).astype(jnp.int32)
    ordered = density[source_rows]
    skeleton = jnp.einsum('tnl,trl->tnr', ordered.astype(jnp.float32), basis_in.astype(jnp.float32)).astype(jnp.bfloat16)
    stacked = skeleton.reshape(NODES, CHILD, NRHS, RANK).transpose(0, 2, 1, 3).reshape(NODES, NRHS, CHILD * RANK)
    node_skel = jnp.einsum('pnk,prk->pnr', stacked.astype(jnp.float32), transfer.astype(jnp.float32)).astype(jnp.bfloat16)
    shaped = geometry.reshape(6, LEAVES, LEAF)
    proxies = shaped[0:3, :, :RANK]
    node_pts = node_points.reshape(3, NODES, RANK)
    leaf_ids = jnp.arange(LEAVES, dtype=jnp.int32)
    node_ids = jnp.arange(NODES, dtype=jnp.int32)
    zero_half = jnp.zeros((), jnp.bfloat16)

    def leaf_far_block(packed):
        target_ids, entries = packed
        usable = entries >= 0
        sources = jnp.where(usable, entries, 0)
        weights = coupling(proxies[:, target_ids][:, :, None, :, None], proxies[:, sources][:, :, :, None, :]).astype(jnp.bfloat16)
        skel_src = jnp.where(usable[:, :, None, None], skeleton[sources], zero_half)
        return jnp.einsum('bsij,bsnj->bni', weights.astype(jnp.float32), skel_src.astype(jnp.float32))
    leaf_far = lax.map(leaf_far_block, (leaf_ids.reshape(-1, 16), far_list.reshape(-1, 16, FAR))).reshape(LEAVES, NRHS, RANK)

    def node_far_block(packed):
        target_ids, entries = packed
        usable = entries >= 0
        sources = jnp.where(usable, entries, 0)
        weights = coupling(node_pts[:, target_ids][:, :, None, :, None], node_pts[:, sources][:, :, :, None, :]).astype(jnp.bfloat16)
        skel_src = jnp.where(usable[:, :, None, None], node_skel[sources], zero_half)
        return jnp.einsum('bsij,bsnj->bni', weights.astype(jnp.float32), skel_src.astype(jnp.float32))
    node_far = lax.map(node_far_block, (node_ids.reshape(-1, 8), node_list.reshape(-1, 8, FAR_NODE))).reshape(NODES, NRHS, RANK).astype(jnp.bfloat16)
    down = jnp.einsum('pnr,prk->pnk', node_far.astype(jnp.float32), transfer.astype(jnp.float32))
    down = down.reshape(NODES, NRHS, CHILD, RANK).transpose(0, 2, 1, 3).reshape(LEAVES, NRHS, RANK)
    local = (leaf_far + down).astype(jnp.bfloat16)
    far_out = jnp.einsum('tnr,trl->tnl', local.astype(jnp.float32), basis_out.astype(jnp.float32))

    def near_block(packed):
        target_ids, entries = packed
        usable = entries >= 0
        sources = jnp.where(usable, entries, 0)
        source_geo = shaped[:, sources]
        kernel = double_layer(shaped[0:3, target_ids][:, :, None, :, None], source_geo[0:3][:, :, :, None, :], source_geo[3:6][:, :, :, None, :]).astype(jnp.bfloat16)
        dens_src = jnp.where(usable[:, :, None, None], ordered[sources], zero_half)
        return jnp.einsum('bsij,bsnj->bni', kernel.astype(jnp.float32), dens_src.astype(jnp.float32))
    near_out = lax.map(near_block, (leaf_ids.reshape(-1, 16), near_list.reshape(-1, 16, NEAR))).reshape(LEAVES, NRHS, LEAF)
    return (near_out + far_out).astype(jnp.bfloat16)
```

```python
import functools
import math

import jax
import jax.numpy as jnp
from jax import lax
from jax.experimental import pallas as pl
from jax.experimental.pallas import tpu as pltpu
from jax.sharding import PartitionSpec as P

REACH = 16
smoothing = 0.1
inv_four_pi = 0.25 / math.pi
NT = (((1,), (1,)), ((), ()))


def extended(cells, sides, width):
    for axis, dim in sides:
        count = lax.axis_size(axis)
        ends = count - 1
        head = lax.slice_in_dim(cells, 0, width, axis=dim)
        tail = lax.slice_in_dim(cells, cells.shape[dim] - width, cells.shape[dim], axis=dim)
        cells = jnp.concatenate(
            [
                lax.ppermute(tail, axis, [(i, (i + 1) % count) for i in range(ends)]),
                cells,
                lax.ppermute(head, axis, [((i + 1) % count, i) for i in range(ends)]),
            ],
            axis=dim,
        )
    return cells


def compacted(entries, base, pad):
    live = entries >= 0
    place = jnp.cumsum(live.astype(jnp.int32), axis=1) - 1
    slots = jnp.arange(entries.shape[1], dtype=jnp.int32)
    hit = live[:, :, None] & (place[:, :, None] == slots)
    return (
        jnp.max(jnp.where(hit, (entries + base)[:, :, None], -1), axis=1),
        pad,
        jnp.sum(live.astype(jnp.int32), axis=1),
    )


def fill(packed):
    rows, pad, count = packed
    return jnp.where(rows < 0, pad, rows), count


def thirds(a):
    high = a.astype(jnp.bfloat16).astype(jnp.float32)
    rest = a - high
    mid = rest.astype(jnp.bfloat16).astype(jnp.float32)
    return high, mid, rest - mid


def left_side(a):
    h, m, l = thirds(a)
    return jnp.concatenate([h, m, h, l, h, m], axis=0)


def right_side(a):
    h, m, l = thirds(a)
    return jnp.concatenate([h, h, m, h, l, m], axis=0)


def point_forms(points, row):
    xyz = jnp.where(row < 3, points, 0.0)
    square = jnp.sum(xyz * xyz, axis=0, keepdims=True)
    target = jnp.where(row < 3, points, jnp.where(row == 3, square, jnp.where(row == 4, 1.0, 0.0)))
    source = jnp.where(
        row < 3,
        -2.0 * points,
        jnp.where(row == 3, 1.0, jnp.where(row == 4, square + smoothing * smoothing, 0.0)),
    )
    return xyz, target, source


def halves(a, lane):
    return jnp.where(lane < 64, a, 0.0), jnp.where(lane < 64, 0.0, pltpu.roll(a, 64, 1))


def field_kernel(
    wide, nodes, chunk,
    near_idx, near_cnt, far_idx, far_cnt, node_idx, node_cnt, first_node,
    geo, dens, skel, node_pts, node_skel, transfer, basis_out, out,
    target_form, source_form, far_form, far_skel, node_target, node_form, node_dens, down,
):
    leaves, nrhs, leaf_size = out.shape
    nodes_here, rank, width = transfer.shape
    children = width // rank
    bf16, f32 = jnp.bfloat16, jnp.float32
    row = lax.broadcasted_iota(jnp.int32, (8, leaf_size), 0)
    lane = lax.broadcasted_iota(jnp.int32, (1, leaf_size), 1)
    low = lane < rank

    def columns(ref, block):
        return ref[:, pl.ds(pl.multiple_of(block * leaf_size, leaf_size), leaf_size)]

    def node_block(b, carry):
        _, _, source = point_forms(columns(node_pts, b), row)
        form = right_side(source)
        turned = pltpu.roll(form, rank, 1)
        node_form[0, 2 * b] = jnp.where(low, form, 0.0).astype(bf16)
        node_form[1, 2 * b] = jnp.where(low, 0.0, turned).astype(bf16)
        node_form[0, 2 * b + 1] = jnp.where(low, turned, 0.0).astype(bf16)
        node_form[1, 2 * b + 1] = jnp.where(low, 0.0, form).astype(bf16)
        return carry

    lax.fori_loop(0, nodes // 2, node_block, 0)
    node_form[0, nodes] = node_form[0, 0]
    node_form[1, nodes] = node_form[1, 0]

    def spread(skel_ref, spread_ref, count):
        def step(s, carry):
            both = jnp.concatenate([skel_ref[s], skel_ref[s]], axis=1)
            none = jnp.zeros_like(both)
            spread_ref[0, s] = jnp.where(low, both, none)
            spread_ref[1, s] = jnp.where(low, none, both)
            return carry

        lax.fori_loop(0, count, step, 0)
        spread_ref[0, count] = jnp.zeros((nrhs, leaf_size), bf16)
        spread_ref[1, count] = jnp.zeros((nrhs, leaf_size), bf16)

    spread(node_skel, node_dens, nodes)
    spread(skel, far_skel, wide)

    for b in range(nodes_here // 2):
        _, target, _ = point_forms(columns(node_pts, first_node[0] // 2 + b), row)
        turned = left_side(target).T.astype(bf16)
        node_target[2 * b] = turned[:rank]
        node_target[2 * b + 1] = turned[rank:]

    def leaf_block(s, carry):
        points = columns(geo, s)
        xyz, target, source = point_forms(points, row)
        normal = jnp.where(row < 3, pltpu.roll(points, 5, 0), 0.0) * inv_four_pi
        shift = -jnp.sum(normal * xyz, axis=0, keepdims=True)
        normal = jnp.where(row == 4, shift, normal)
        form = right_side(source)
        source_form[s] = jnp.concatenate([form, right_side(normal)], axis=1).astype(bf16)
        far_form[0, s] = jnp.where(low, form, 0.0).astype(bf16)
        far_form[1, s] = jnp.where(low, 0.0, pltpu.roll(form, rank, 1)).astype(bf16)
        return carry

    lax.fori_loop(0, wide, leaf_block, 0)
    source_form[wide] = source_form[0]
    far_form[0, wide] = far_form[0, 0]
    far_form[1, wide] = far_form[1, 0]

    def own_block(t, carry):
        _, target, _ = point_forms(columns(geo, t + REACH), row)
        target_form[t] = left_side(target).T.astype(bf16)
        return carry

    lax.fori_loop(0, leaves, own_block, 0)

    def coupled(idx, count, t, form, points, charges):
        def step(c, acc):
            ids = [idx[t, c * chunk + k] for k in range(chunk)]
            weights = jnp.concatenate(
                [points[0, ids[k]] + points[1, ids[k + 1]] for k in range(0, chunk, 2)], axis=1
            )
            square = jnp.dot(form, weights, preferred_element_type=f32)
            kernel = (inv_four_pi * lax.rsqrt(square)).astype(bf16)
            charge = jnp.concatenate(
                [charges[0, ids[k]] + charges[1, ids[k + 1]] for k in range(0, chunk, 2)], axis=1
            )
            return acc + lax.dot_general(charge, kernel, NT, preferred_element_type=f32)

        return lax.fori_loop(0, (count[t] + chunk - 1) // chunk, step, jnp.zeros((nrhs, rank), f32))

    for p in range(nodes_here):
        far = coupled(node_idx, node_cnt, p, node_target[p], node_form, node_dens).astype(bf16)
        spreading = jnp.dot(far, transfer[p], preferred_element_type=f32)
        for c in range(children):
            down[p * children + c] = spreading[:, c * rank : (c + 1) * rank]

    def leaf(t, carry):
        form = target_form[t]
        far = coupled(far_idx, far_cnt, t, form[:rank], far_form, far_skel)
        local = (far + down[t]).astype(bf16)
        start = jnp.dot(local, basis_out[t], preferred_element_type=f32)

        def step(c, acc):
            kernels, charges = [], []
            for k in range(chunk):
                s = near_idx[t, c * chunk + k]
                both = jnp.dot(form, source_form[s], preferred_element_type=f32)
                r = lax.rsqrt(both[:, :leaf_size])
                kernels.append((both[:, leaf_size:] * (r * r * r)).astype(bf16))
                charges.append(dens[s])
            return acc + lax.dot_general(
                jnp.concatenate(charges, axis=1),
                jnp.concatenate(kernels, axis=1),
                NT,
                preferred_element_type=f32,
            )

        out[t] = lax.fori_loop(0, (near_cnt[t] + chunk - 1) // chunk, step, start).astype(bf16)
        return carry

    lax.fori_loop(0, leaves, leaf, 0)


def field(near, far, node, first_node, geo, dens, skel, node_pts, node_skel, transfer, basis_out):
    wide, nodes = skel.shape[0], node_skel.shape[0]
    nrhs, leaf_size = dens.shape[1:]
    nodes_here, rank, width = transfer.shape
    leaves = basis_out.shape[0]
    terms = 48
    bf16 = jnp.bfloat16
    smem = pl.BlockSpec(memory_space=pltpu.SMEM)
    vmem = pl.BlockSpec(memory_space=pltpu.VMEM)
    return pl.pallas_call(
        functools.partial(field_kernel, wide, nodes, 4),
        out_shape=jax.ShapeDtypeStruct((leaves, nrhs, leaf_size), bf16),
        in_specs=[smem] * 7 + [vmem] * 7,
        out_specs=vmem,
        scratch_shapes=[
            pltpu.VMEM((leaves, leaf_size, terms), bf16),
            pltpu.VMEM((wide + 1, terms, 2 * leaf_size), bf16),
            pltpu.VMEM((2, wide + 1, terms, leaf_size), bf16),
            pltpu.VMEM((2, wide + 1, nrhs, leaf_size), bf16),
            pltpu.VMEM((nodes_here, rank, terms), bf16),
            pltpu.VMEM((2, nodes + 1, terms, leaf_size), bf16),
            pltpu.VMEM((2, nodes + 1, nrhs, leaf_size), bf16),
            pltpu.VMEM((leaves, nrhs, rank), jnp.float32),
        ],
        compiler_params=pltpu.CompilerParams(vmem_limit_bytes=48 * 1024 * 1024),
        name="field",
    )(*near, *far, *node, first_node, geo, dens, skel, node_pts, node_skel, transfer, basis_out)


def on_device(
    density,
    leaf_target,
    geometry,
    near_list,
    far_list,
    node_list,
    basis_in,
    basis_out,
    transfer,
    node_points,
):
    leaves, nrhs_here, leaf_size = density.shape
    rank_size = basis_in.shape[1]
    nodes_here = transfer.shape[0]
    children = leaves // nodes_here
    wide = leaves + 2 * REACH
    first_leaf = lax.axis_index(("row", "col")) * leaves
    destination = leaf_target // leaves
    tree_slot = leaf_target % leaves
    send_order = jnp.argsort(destination, stable=True)
    outgoing = density[send_order]
    out_slot = tree_slot[send_order]
    arrived, arrived_slot = (
        lax.all_to_all(outgoing, ("row", "col"), split_axis=0, concat_axis=0, tiled=True),
        lax.all_to_all(out_slot, ("row", "col"), split_axis=0, concat_axis=0, tiled=True),
    )
    ordered = arrived[jnp.argsort(arrived_slot)]
    geo_wide = extended(
        jnp.pad(geometry, ((0, 2), (0, 0))), ((("row", "col"), 1),), REACH * leaf_size
    )
    skeleton = jnp.einsum(
        "tnl,trl->tnr", ordered, basis_in, preferred_element_type=jnp.float32
    ).astype(jnp.bfloat16)
    dens_wide = extended(ordered, ((("row", "col"), 0),), REACH)
    dens_wide = jnp.pad(dens_wide, ((0, 1), (0, 0), (0, 0)))
    skel_wide = extended(skeleton, ((("row", "col"), 0),), REACH)
    stacked = (
        skeleton.reshape(nodes_here, children, nrhs_here, rank_size)
        .transpose(0, 2, 1, 3)
        .reshape(nodes_here, nrhs_here, children * rank_size)
    )
    node_skel = jnp.einsum(
        "pnk,prk->pnr", stacked, transfer, preferred_element_type=jnp.float32
    ).astype(jnp.bfloat16)
    all_skel = lax.all_gather(
        node_skel.reshape(nodes_here, nrhs_here * rank_size), ("row", "col"), axis=0, tiled=True
    ).reshape(-1, nrhs_here, rank_size)
    nodes = all_skel.shape[0]
    near = fill(compacted(near_list, REACH - first_leaf, wide))
    far = fill(compacted(far_list, REACH - first_leaf, wide))
    node = fill(compacted(node_list, 0, nodes))
    first_node = (first_leaf // children).reshape(1)
    node_pts = jnp.pad(node_points, ((0, 5), (0, 0)))
    return field(
        near, far, node, first_node, geo_wide, dens_wide, skel_wide, node_pts, all_skel,
        transfer, basis_out,
    )


def solution(mesh):
    return jax.shard_map(
        on_device,
        mesh=mesh,
        in_specs=(
            P(("grp", "row", "col"), None, None),
            P(("grp", "row", "col")),
            P(None, ("grp", "row", "col")),
            P(("grp", "row", "col"), None),
            P(("grp", "row", "col"), None),
            P(("grp", "row", "col"), None),
            P(("grp", "row", "col"), None, None),
            P(("grp", "row", "col"), None, None),
            P(("grp", "row", "col"), None, None),
            P(None, "grp"),
        ),
        out_specs=P(("grp", "row", "col"), None, None),
        check_vma=False,
    )
```

```python
import functools
import math

import jax
import jax.numpy as jnp
from jax import lax
from jax.experimental import pallas as pl
from jax.experimental.pallas import tpu as pltpu
from jax.sharding import PartitionSpec as P

REACH = 16
smoothing = 0.1
inv_four_pi = 0.25 / math.pi
NT = (((1,), (1,)), ((), ()))


def extended(cells, sides, width):
    for axis, dim in sides:
        count = lax.axis_size(axis)
        ends = count - 1
        head = lax.slice_in_dim(cells, 0, width, axis=dim)
        tail = lax.slice_in_dim(cells, cells.shape[dim] - width, cells.shape[dim], axis=dim)
        cells = jnp.concatenate(
            [
                lax.ppermute(tail, axis, [(i, (i + 1) % count) for i in range(ends)]),
                cells,
                lax.ppermute(head, axis, [((i + 1) % count, i) for i in range(ends)]),
            ],
            axis=dim,
        )
    return cells


def compacted(entries, base, pad):
    live = entries >= 0
    place = jnp.cumsum(live.astype(jnp.int32), axis=1) - 1
    slots = jnp.arange(entries.shape[1], dtype=jnp.int32)
    hit = live[:, :, None] & (place[:, :, None] == slots)
    return (
        jnp.max(jnp.where(hit, (entries + base)[:, :, None], -1), axis=1),
        pad,
        jnp.sum(live.astype(jnp.int32), axis=1),
    )


def fill(packed):
    rows, pad, count = packed
    return jnp.where(rows < 0, pad, rows), count


def thirds(a):
    high = a.astype(jnp.bfloat16).astype(jnp.float32)
    rest = a - high
    mid = rest.astype(jnp.bfloat16).astype(jnp.float32)
    return high, mid, rest - mid


def left_side(a):
    h, m, l = thirds(a)
    return jnp.concatenate([h, m, h, l, h, m], axis=0)


def right_side(a):
    h, m, l = thirds(a)
    return jnp.concatenate([h, h, m, h, l, m], axis=0)


def point_forms(points, row):
    xyz = jnp.where(row < 3, points, 0.0)
    square = jnp.sum(xyz * xyz, axis=0, keepdims=True)
    target = jnp.where(row < 3, points, jnp.where(row == 3, square, jnp.where(row == 4, 1.0, 0.0)))
    source = jnp.where(
        row < 3,
        -2.0 * points,
        jnp.where(row == 3, 1.0, jnp.where(row == 4, square + smoothing * smoothing, 0.0)),
    )
    return xyz, target, source


def flat(count, chunk, size):
    rows = count.shape[0]
    chunks = (count + chunk - 1) // chunk
    row_ids = jnp.arange(rows, dtype=jnp.int32)
    end = jnp.sum(jnp.where(row_ids[:, None] >= row_ids, chunks, 0), axis=1)
    g = jnp.arange(size, dtype=jnp.int32)
    row = jnp.sum((end <= g[:, None]).astype(jnp.int32), axis=1)
    start = jnp.sum(jnp.where(row_ids == row[:, None], end - chunks, 0), axis=1)
    return row, jnp.where(row < rows, (g - start) * chunk, 0), jnp.sum(chunks).reshape(1)


def field_kernel(
    wide, nodes, chunk,
    near_idx, near_row, near_col, near_total, far_idx, far_row, far_col, far_total, first_node,
    geo, dens, skel, node_pts, node_skel, transfer, basis_out, out,
    target_form, source_form, far_target, far_form, far_skel, near_acc, far_acc, both, near_k, square, far_k,
):
    leaves, nrhs, leaf_size = out.shape
    nodes_here, rank, width = transfer.shape
    children = width // rank
    bf16, f32 = jnp.bfloat16, jnp.float32
    row = lax.broadcasted_iota(jnp.int32, (8, leaf_size), 0)
    lane = lax.broadcasted_iota(jnp.int32, (1, leaf_size), 1)
    low = lane < rank
    base = wide + 1
    group = 4

    def columns(ref, block):
        return ref[:, pl.ds(pl.multiple_of(block * leaf_size, leaf_size), leaf_size)]

    def each(count, body):
        def step(i, carry):
            for k in range(group):
                body(i * group + k)
            return carry

        lax.fori_loop(0, count // group, step, 0)

    def node_block(b):
        _, _, source = point_forms(columns(node_pts, b), row)
        form = right_side(source)
        turned = pltpu.roll(form, rank, 1)
        far_form[0, base + 2 * b] = jnp.where(low, form, 0.0).astype(bf16)
        far_form[1, base + 2 * b] = jnp.where(low, 0.0, turned).astype(bf16)
        far_form[0, base + 2 * b + 1] = jnp.where(low, turned, 0.0).astype(bf16)
        far_form[1, base + 2 * b + 1] = jnp.where(low, 0.0, form).astype(bf16)

    each(nodes // 2, node_block)

    def spread(skel_ref, first):
        def step(s):
            both_halves = jnp.concatenate([skel_ref[s], skel_ref[s]], axis=1)
            none = jnp.zeros_like(both_halves)
            far_skel[0, first + s] = jnp.where(low, both_halves, none)
            far_skel[1, first + s] = jnp.where(low, none, both_halves)

        each(skel_ref.shape[0], step)

    spread(node_skel, base)
    spread(skel, 0)
    far_skel[0, wide] = jnp.zeros((nrhs, leaf_size), bf16)
    far_skel[1, wide] = jnp.zeros((nrhs, leaf_size), bf16)

    for b in range(nodes_here // 2):
        _, target, _ = point_forms(columns(node_pts, first_node[0] // 2 + b), row)
        turned = left_side(target).T.astype(bf16)
        far_target[leaves + 2 * b] = turned[:rank]
        far_target[leaves + 2 * b + 1] = turned[rank:]

    def leaf_block(s):
        points = columns(geo, s)
        xyz, target, source = point_forms(points, row)
        normal = jnp.where(row < 3, pltpu.roll(points, 5, 0), 0.0) * inv_four_pi
        shift = -jnp.sum(normal * xyz, axis=0, keepdims=True)
        normal = jnp.where(row == 4, shift, normal)
        form = right_side(source)
        source_form[s] = jnp.concatenate([form, right_side(normal)], axis=1).astype(bf16)
        far_form[0, s] = jnp.where(low, form, 0.0).astype(bf16)
        far_form[1, s] = jnp.where(low, 0.0, pltpu.roll(form, rank, 1)).astype(bf16)

    each(wide, leaf_block)
    source_form[wide] = source_form[0]
    far_form[0, wide] = far_form[0, 0]
    far_form[1, wide] = far_form[1, 0]

    def own_block(t):
        _, target, _ = point_forms(columns(geo, t + REACH), row)
        turned = left_side(target).T.astype(bf16)
        target_form[t] = turned
        far_target[t] = turned[:rank]
        near_acc[t] = jnp.zeros((nrhs, leaf_size), f32)
        far_acc[t] = jnp.zeros((nrhs, rank), f32)

    each(leaves, own_block)
    for p in range(nodes_here):
        far_acc[leaves + p] = jnp.zeros((nrhs, rank), f32)

    def pipeline(idx, rows_of, cols_of, total, rows, first, middle, last):
        def ids_of(g):
            t, c = jnp.minimum(rows_of[g], rows - 1), cols_of[g]
            return t, [idx[t, c + k] for k in range(chunk)]

        def step(g, carry):
            old = jnp.maximum(g - 2, 0)
            last(jnp.where(g >= 2, rows_of[old], rows), ids_of(old)[1])
            middle()
            first(*ids_of(g))
            return carry

        lax.fori_loop(0, total[0] + 2, step, 0)

    def far_first(t, ids):
        weights = jnp.concatenate(
            [far_form[0, ids[k]] + far_form[1, ids[k + 1]] for k in range(0, chunk, 2)], axis=1
        )
        square[...] = jnp.dot(far_target[t], weights, preferred_element_type=f32)

    def far_middle():
        far_k[...] = (inv_four_pi * lax.rsqrt(square[...])).astype(bf16)

    def far_last(t, ids):
        charge = jnp.concatenate(
            [far_skel[0, ids[k]] + far_skel[1, ids[k + 1]] for k in range(0, chunk, 2)], axis=1
        )
        far_acc[t] += lax.dot_general(charge, far_k[...], NT, preferred_element_type=f32)

    pipeline(
        far_idx, far_row, far_col, far_total, leaves + nodes_here, far_first, far_middle, far_last
    )

    def near_first(t, ids):
        form = target_form[t]
        for k in range(chunk):
            both[k] = jnp.dot(form, source_form[ids[k]], preferred_element_type=f32)

    def near_middle():
        for k in range(chunk):
            r = lax.rsqrt(both[k, :, :leaf_size])
            near_k[:, k * leaf_size : (k + 1) * leaf_size] = (
                both[k, :, leaf_size:] * (r * r * r)
            ).astype(bf16)

    def near_last(t, ids):
        charge = jnp.concatenate([dens[ids[k]] for k in range(chunk)], axis=1)
        near_acc[t] += lax.dot_general(charge, near_k[...], NT, preferred_element_type=f32)

    pipeline(
        near_idx, near_row, near_col, near_total, leaves, near_first, near_middle, near_last
    )

    for p in range(nodes_here):
        far = far_acc[leaves + p].astype(bf16)
        spreading = jnp.dot(far, transfer[p], preferred_element_type=f32)
        for c in range(children):
            t = p * children + c
            local = (far_acc[t] + spreading[:, c * rank : (c + 1) * rank]).astype(bf16)
            out[t] = (
                near_acc[t] + jnp.dot(local, basis_out[t], preferred_element_type=f32)
            ).astype(bf16)


def field(near, far, node, first_node, geo, dens, skel, node_pts, node_skel, transfer, basis_out):
    wide, nodes = skel.shape[0], node_skel.shape[0]
    nrhs, leaf_size = dens.shape[1:]
    nodes_here, rank, width = transfer.shape
    leaves = basis_out.shape[0]
    terms, chunk = 48, 4
    bf16, f32 = jnp.bfloat16, jnp.float32
    near_idx, near_count = near
    far_idx, far_count = far
    node_idx, node_count = node
    slots = node_idx.shape[1]
    far_size = (far_idx.size + node_idx.size) // chunk + 2
    far_idx = jnp.concatenate(
        [
            jnp.pad(far_idx, ((0, 0), (0, slots - far_idx.shape[1])), constant_values=wide),
            node_idx,
        ],
        axis=0,
    )
    far_count = jnp.concatenate([far_count, node_count])
    smem = pl.BlockSpec(memory_space=pltpu.SMEM)
    vmem = pl.BlockSpec(memory_space=pltpu.VMEM)
    return pl.pallas_call(
        functools.partial(field_kernel, wide, nodes, chunk),
        out_shape=jax.ShapeDtypeStruct((leaves, nrhs, leaf_size), bf16),
        in_specs=[smem] * 9 + [vmem] * 7,
        out_specs=vmem,
        scratch_shapes=[
            pltpu.VMEM((leaves, leaf_size, terms), bf16),
            pltpu.VMEM((wide + 1, terms, 2 * leaf_size), bf16),
            pltpu.VMEM((leaves + nodes_here, rank, terms), bf16),
            pltpu.VMEM((2, wide + 1 + nodes, terms, leaf_size), bf16),
            pltpu.VMEM((2, wide + 1 + nodes, nrhs, leaf_size), bf16),
            pltpu.VMEM((leaves + 1, nrhs, leaf_size), f32),
            pltpu.VMEM((leaves + nodes_here + 1, nrhs, rank), f32),
            pltpu.VMEM((chunk, leaf_size, 2 * leaf_size), f32),
            pltpu.VMEM((leaf_size, chunk * leaf_size), bf16),
            pltpu.VMEM((rank, chunk * rank), f32),
            pltpu.VMEM((rank, chunk * rank), bf16),
        ],
        compiler_params=pltpu.CompilerParams(vmem_limit_bytes=48 * 1024 * 1024),
        name="field",
    )(
        near_idx, *flat(near_count, chunk, near_idx.size // chunk + 2),
        far_idx, *flat(far_count, chunk, far_size),
        first_node, geo, dens, skel, node_pts, node_skel, transfer, basis_out,
    )


def on_device(
    density,
    leaf_target,
    geometry,
    near_list,
    far_list,
    node_list,
    basis_in,
    basis_out,
    transfer,
    node_points,
):
    leaves, nrhs_here, leaf_size = density.shape
    rank_size = basis_in.shape[1]
    nodes_here = transfer.shape[0]
    children = leaves // nodes_here
    wide = leaves + 2 * REACH
    first_leaf = lax.axis_index(("row", "col")) * leaves
    destination = leaf_target // leaves
    tree_slot = leaf_target % leaves
    send_order = jnp.argsort(destination, stable=True)
    outgoing = density[send_order]
    out_slot = tree_slot[send_order]
    arrived, arrived_slot = (
        lax.all_to_all(outgoing, ("row", "col"), split_axis=0, concat_axis=0, tiled=True),
        lax.all_to_all(out_slot, ("row", "col"), split_axis=0, concat_axis=0, tiled=True),
    )
    ordered = arrived[jnp.argsort(arrived_slot)]
    geo_wide = extended(
        jnp.pad(geometry, ((0, 2), (0, 0))), ((("row", "col"), 1),), REACH * leaf_size
    )
    skeleton = jnp.einsum(
        "tnl,trl->tnr", ordered, basis_in, preferred_element_type=jnp.float32
    ).astype(jnp.bfloat16)
    dens_wide = extended(ordered, ((("row", "col"), 0),), REACH)
    dens_wide = jnp.pad(dens_wide, ((0, 1), (0, 0), (0, 0)))
    skel_wide = extended(skeleton, ((("row", "col"), 0),), REACH)
    stacked = (
        skeleton.reshape(nodes_here, children, nrhs_here, rank_size)
        .transpose(0, 2, 1, 3)
        .reshape(nodes_here, nrhs_here, children * rank_size)
    )
    node_skel = jnp.einsum(
        "pnk,prk->pnr", stacked, transfer, preferred_element_type=jnp.float32
    ).astype(jnp.bfloat16)
    all_skel = lax.all_gather(
        node_skel.reshape(nodes_here, nrhs_here * rank_size), ("row", "col"), axis=0, tiled=True
    ).reshape(-1, nrhs_here, rank_size)
    near = fill(compacted(near_list, REACH - first_leaf, wide))
    far = fill(compacted(far_list, REACH - first_leaf, wide))
    node = fill(compacted(node_list, wide + 1, wide))
    first_node = (first_leaf // children).reshape(1)
    node_pts = jnp.pad(node_points, ((0, 5), (0, 0)))
    return field(
        near, far, node, first_node, geo_wide, dens_wide, skel_wide, node_pts, all_skel,
        transfer, basis_out,
    )


def solution(mesh):
    return jax.shard_map(
        on_device,
        mesh=mesh,
        in_specs=(
            P(("grp", "row", "col"), None, None),
            P(("grp", "row", "col")),
            P(None, ("grp", "row", "col")),
            P(("grp", "row", "col"), None),
            P(("grp", "row", "col"), None),
            P(("grp", "row", "col"), None),
            P(("grp", "row", "col"), None, None),
            P(("grp", "row", "col"), None, None),
            P(("grp", "row", "col"), None, None),
            P(None, "grp"),
        ),
        out_specs=P(("grp", "row", "col"), None, None),
        check_vma=False,
    )
```

```python
import functools
import math

import jax
import jax.numpy as jnp
from jax import lax
from jax.experimental import pallas as pl
from jax.experimental.pallas import tpu as pltpu
from jax.sharding import PartitionSpec as P

REACH = 16
smoothing = 0.1
inv_four_pi = 0.25 / math.pi
NT = (((1,), (1,)), ((), ()))


def compacted(entries, base, pad):
    live = entries >= 0
    place = jnp.cumsum(live.astype(jnp.int32), axis=1) - 1
    slots = jnp.arange(entries.shape[1], dtype=jnp.int32)
    hit = live[:, :, None] & (place[:, :, None] == slots)
    return (
        jnp.max(jnp.where(hit, (entries + base)[:, :, None], -1), axis=1),
        pad,
        jnp.sum(live.astype(jnp.int32), axis=1),
    )


def fill(packed):
    rows, pad, count = packed
    return jnp.where(rows < 0, pad, rows), count


def thirds(a):
    high = a.astype(jnp.bfloat16).astype(jnp.float32)
    rest = a - high
    mid = rest.astype(jnp.bfloat16).astype(jnp.float32)
    return high, mid, rest - mid


def left_side(a):
    h, m, l = thirds(a)
    return jnp.concatenate([h, m, h, l, h, m], axis=0)


def right_side(a):
    h, m, l = thirds(a)
    return jnp.concatenate([h, h, m, h, l, m], axis=0)


def point_forms(points, row):
    xyz = jnp.where(row < 3, points, 0.0)
    square = jnp.sum(xyz * xyz, axis=0, keepdims=True)
    target = jnp.where(row < 3, points, jnp.where(row == 3, square, jnp.where(row == 4, 1.0, 0.0)))
    source = jnp.where(
        row < 3,
        -2.0 * points,
        jnp.where(row == 3, 1.0, jnp.where(row == 4, square + smoothing * smoothing, 0.0)),
    )
    return xyz, target, source


def flat(count, chunk, size):
    rows = count.shape[0]
    chunks = (count + chunk - 1) // chunk
    row_ids = jnp.arange(rows, dtype=jnp.int32)
    end = jnp.sum(jnp.where(row_ids[:, None] >= row_ids, chunks, 0), axis=1)
    g = jnp.arange(size, dtype=jnp.int32)
    row = jnp.sum((end <= g[:, None]).astype(jnp.int32), axis=1)
    start = jnp.sum(jnp.where(row_ids == row[:, None], end - chunks, 0), axis=1)
    return row, jnp.where(row < rows, (g - start) * chunk, 0), jnp.sum(chunks).reshape(1)


def field_kernel(
    wide, nodes, chunk,
    near_idx, near_row, near_col, near_total, far_idx, far_row, far_col, far_total, first_node,
    geo, dens, skel, node_pts, node_skel, transfer, basis_out, out,
    target_form, source_form, far_target, far_form, far_skel, near_acc, far_acc, both, near_k, square, far_k,
):
    leaves, nrhs, leaf_size = out.shape
    nodes_here, rank, width = transfer.shape
    children = width // rank
    bf16, f32 = jnp.bfloat16, jnp.float32
    row = lax.broadcasted_iota(jnp.int32, (8, leaf_size), 0)
    lane = lax.broadcasted_iota(jnp.int32, (1, leaf_size), 1)
    low = lane < rank
    base = wide + 1
    group = 4

    def columns(ref, block):
        return ref[:, pl.ds(pl.multiple_of(block * leaf_size, leaf_size), leaf_size)]

    def each(count, body):
        def step(i, carry):
            for k in range(group):
                body(i * group + k)
            return carry

        lax.fori_loop(0, count // group, step, 0)

    def node_block(b):
        _, _, source = point_forms(columns(node_pts, b), row)
        form = right_side(source)
        turned = pltpu.roll(form, rank, 1)
        far_form[0, base + 2 * b] = jnp.where(low, form, 0.0).astype(bf16)
        far_form[1, base + 2 * b] = jnp.where(low, 0.0, turned).astype(bf16)
        far_form[0, base + 2 * b + 1] = jnp.where(low, turned, 0.0).astype(bf16)
        far_form[1, base + 2 * b + 1] = jnp.where(low, 0.0, form).astype(bf16)

    each(nodes // 2, node_block)

    def spread(skel_ref, first):
        def step(s):
            both_halves = jnp.concatenate([skel_ref[s], skel_ref[s]], axis=1)
            none = jnp.zeros_like(both_halves)
            far_skel[0, first + s] = jnp.where(low, both_halves, none)
            far_skel[1, first + s] = jnp.where(low, none, both_halves)

        each(skel_ref.shape[0], step)

    spread(node_skel, base)
    spread(skel, 0)
    far_skel[0, wide] = jnp.zeros((nrhs, leaf_size), bf16)
    far_skel[1, wide] = jnp.zeros((nrhs, leaf_size), bf16)

    for b in range(nodes_here // 2):
        _, target, _ = point_forms(columns(node_pts, first_node[0] // 2 + b), row)
        turned = left_side(target).T.astype(bf16)
        far_target[leaves + 2 * b] = turned[:rank]
        far_target[leaves + 2 * b + 1] = turned[rank:]

    def leaf_block(s):
        points = columns(geo, s)
        xyz, target, source = point_forms(points, row)
        normal = jnp.where(row < 3, pltpu.roll(points, 5, 0), 0.0) * inv_four_pi
        shift = -jnp.sum(normal * xyz, axis=0, keepdims=True)
        normal = jnp.where(row == 4, shift, normal)
        form = right_side(source)
        source_form[s] = jnp.concatenate([form, right_side(normal)], axis=1).astype(bf16)
        far_form[0, s] = jnp.where(low, form, 0.0).astype(bf16)
        far_form[1, s] = jnp.where(low, 0.0, pltpu.roll(form, rank, 1)).astype(bf16)

    each(wide, leaf_block)
    source_form[wide] = source_form[0]
    far_form[0, wide] = far_form[0, 0]
    far_form[1, wide] = far_form[1, 0]

    def own_block(t):
        _, target, _ = point_forms(columns(geo, t + REACH), row)
        turned = left_side(target).T.astype(bf16)
        target_form[t] = turned
        far_target[t] = turned[:rank]
        near_acc[t] = jnp.zeros((nrhs, leaf_size), f32)
        far_acc[t] = jnp.zeros((nrhs, rank), f32)

    each(leaves, own_block)
    for p in range(nodes_here):
        far_acc[leaves + p] = jnp.zeros((nrhs, rank), f32)

    def pipeline(idx, rows_of, cols_of, total, rows, first, middle, last):
        def ids_of(g):
            t, c = jnp.minimum(rows_of[g], rows - 1), cols_of[g]
            return t, [idx[t, c + k] for k in range(chunk)]

        def step(g, carry):
            old = jnp.maximum(g - 2, 0)
            last(jnp.where(g >= 2, rows_of[old], rows), ids_of(old)[1])
            middle()
            first(*ids_of(g))
            return carry

        lax.fori_loop(0, total[0] + 2, step, 0)

    def far_first(t, ids):
        weights = jnp.concatenate(
            [far_form[0, ids[k]] + far_form[1, ids[k + 1]] for k in range(0, chunk, 2)], axis=1
        )
        square[...] = jnp.dot(far_target[t], weights, preferred_element_type=f32)

    def far_middle():
        far_k[...] = (inv_four_pi * lax.rsqrt(square[...])).astype(bf16)

    def far_last(t, ids):
        charge = jnp.concatenate(
            [far_skel[0, ids[k]] + far_skel[1, ids[k + 1]] for k in range(0, chunk, 2)], axis=1
        )
        far_acc[t] += lax.dot_general(charge, far_k[...], NT, preferred_element_type=f32)

    pipeline(
        far_idx, far_row, far_col, far_total, leaves + nodes_here, far_first, far_middle, far_last
    )

    def near_first(t, ids):
        form = target_form[t]
        for k in range(chunk):
            both[k] = jnp.dot(form, source_form[ids[k]], preferred_element_type=f32)

    def near_middle():
        for k in range(chunk):
            r = lax.rsqrt(both[k, :, :leaf_size])
            near_k[:, k * leaf_size : (k + 1) * leaf_size] = (
                both[k, :, leaf_size:] * (r * r * r)
            ).astype(bf16)

    def near_last(t, ids):
        charge = jnp.concatenate([dens[ids[k]] for k in range(chunk)], axis=1)
        near_acc[t] += lax.dot_general(charge, near_k[...], NT, preferred_element_type=f32)

    pipeline(
        near_idx, near_row, near_col, near_total, leaves, near_first, near_middle, near_last
    )

    for p in range(nodes_here):
        far = far_acc[leaves + p].astype(bf16)
        spreading = jnp.dot(far, transfer[p], preferred_element_type=f32)
        for c in range(children):
            t = p * children + c
            local = (far_acc[t] + spreading[:, c * rank : (c + 1) * rank]).astype(bf16)
            out[t] = (
                near_acc[t] + jnp.dot(local, basis_out[t], preferred_element_type=f32)
            ).astype(bf16)


def field(near, far, node, first_node, geo, dens, skel, node_pts, node_skel, transfer, basis_out):
    wide, nodes = skel.shape[0], node_skel.shape[0]
    nrhs, leaf_size = dens.shape[1:]
    nodes_here, rank, width = transfer.shape
    leaves = basis_out.shape[0]
    terms, chunk = 48, 4
    bf16, f32 = jnp.bfloat16, jnp.float32
    near_idx, near_count = near
    far_idx, far_count = far
    node_idx, node_count = node
    slots = node_idx.shape[1]
    far_size = (far_idx.size + node_idx.size) // chunk + 2
    far_idx = jnp.concatenate(
        [
            jnp.pad(far_idx, ((0, 0), (0, slots - far_idx.shape[1])), constant_values=wide),
            node_idx,
        ],
        axis=0,
    )
    far_count = jnp.concatenate([far_count, node_count])
    smem = pl.BlockSpec(memory_space=pltpu.SMEM)
    vmem = pl.BlockSpec(memory_space=pltpu.VMEM)
    return pl.pallas_call(
        functools.partial(field_kernel, wide, nodes, chunk),
        out_shape=jax.ShapeDtypeStruct((leaves, nrhs, leaf_size), bf16),
        in_specs=[smem] * 9 + [vmem] * 7,
        out_specs=vmem,
        scratch_shapes=[
            pltpu.VMEM((leaves, leaf_size, terms), bf16),
            pltpu.VMEM((wide + 1, terms, 2 * leaf_size), bf16),
            pltpu.VMEM((leaves + nodes_here, rank, terms), bf16),
            pltpu.VMEM((2, wide + 1 + nodes, terms, leaf_size), bf16),
            pltpu.VMEM((2, wide + 1 + nodes, nrhs, leaf_size), bf16),
            pltpu.VMEM((leaves + 1, nrhs, leaf_size), f32),
            pltpu.VMEM((leaves + nodes_here + 1, nrhs, rank), f32),
            pltpu.VMEM((chunk, leaf_size, 2 * leaf_size), f32),
            pltpu.VMEM((leaf_size, chunk * leaf_size), bf16),
            pltpu.VMEM((rank, chunk * rank), f32),
            pltpu.VMEM((rank, chunk * rank), bf16),
        ],
        compiler_params=pltpu.CompilerParams(vmem_limit_bytes=48 * 1024 * 1024),
        name="field",
    )(
        near_idx, *flat(near_count, chunk, near_idx.size // chunk + 2),
        far_idx, *flat(far_count, chunk, far_size),
        first_node, geo, dens, skel, node_pts, node_skel, transfer, basis_out,
    )


def peers():
    columns = lax.axis_size("col")
    count = lax.axis_size("row") * columns
    me = lax.axis_index("row") * columns + lax.axis_index("col")

    def peer(k):
        q = lax.rem(me + k, count)
        return q, {"row": q // columns, "col": lax.rem(q, columns)}

    return me, count, peer


def greet(count, peer):
    barrier = pltpu.get_barrier_semaphore()
    for k in range(1, count):
        pl.semaphore_signal(
            barrier, inc=1, device_id=peer(k)[1], device_id_type=pl.DeviceIdType.MESH
        )
    pl.semaphore_wait(barrier, count - 1)


def sender(send_sem, recv_sem):
    copies = []

    def send(src, dst, where):
        k = len(copies)
        copy = pltpu.make_async_remote_copy(
            src_ref=src,
            dst_ref=dst,
            send_sem=send_sem.at[k],
            recv_sem=recv_sem.at[k],
            device_id=where,
            device_id_type=pl.DeviceIdType.MESH,
        )
        copy.start()
        copies.append(copy)

    return copies, send


def exchange_kernel(outgoing, slots, geo, arrived, arrived_slots, geo_wide, send_sem, recv_sem):
    me, count, peer = peers()
    per = outgoing.shape[0] // count
    inner = geo.shape[1]
    halo = (geo_wide.shape[1] - inner) // 2
    greet(count, peer)
    copies, send = sender(send_sem, recv_sem)
    for k in range(1, count):
        q, where = peer(k)
        send(slots.at[q], arrived_slots.at[me], where)
        send(outgoing.at[pl.ds(q * per, per)], arrived.at[pl.ds(me * per, per)], where)
    send(geo.at[:, pl.ds(inner - halo, halo)], geo_wide.at[:, pl.ds(0, halo)], peer(1)[1])
    send(geo.at[:, pl.ds(0, halo)], geo_wide.at[:, pl.ds(halo + inner, halo)], peer(count - 1)[1])
    arrived_slots[me] = slots[me]
    for k in range(per):
        arrived[me * per + k] = outgoing[me * per + k]
    geo_wide[:, halo : halo + inner] = geo[...]
    for copy in copies:
        copy.wait()


def share_kernel(dens, skel, node_skel, dens_wide, skel_wide, all_skel, send_sem, recv_sem):
    me, count, peer = peers()
    leaves, here = dens.shape[0], node_skel.shape[0]
    greet(count, peer)
    copies, send = sender(send_sem, recv_sem)
    for own, wide in ((dens, dens_wide), (skel, skel_wide)):
        send(own.at[pl.ds(leaves - REACH, REACH)], wide.at[pl.ds(0, REACH)], peer(1)[1])
        send(own.at[pl.ds(0, REACH)], wide.at[pl.ds(REACH + leaves, REACH)], peer(count - 1)[1])
    for k in range(1, count):
        send(node_skel, all_skel.at[pl.ds(me * here, here)], peer(k)[1])
    dens_wide[REACH : REACH + leaves] = dens[...]
    dens_wide[leaves + 2 * REACH] = jnp.zeros(dens.shape[1:], dens.dtype)
    skel_wide[REACH : REACH + leaves] = skel[...]
    for k in range(here):
        all_skel[me * here + k] = node_skel[k]
    for copy in copies:
        copy.wait()


def remote(kernel, name, number, copies, outs, *operands):
    vmem = pl.BlockSpec(memory_space=pltpu.VMEM)
    return pl.pallas_call(
        kernel,
        out_shape=[jax.ShapeDtypeStruct(*o) for o in outs],
        in_specs=[vmem] * len(operands),
        out_specs=[vmem] * len(outs),
        scratch_shapes=[pltpu.SemaphoreType.DMA((copies,)), pltpu.SemaphoreType.DMA((copies,))],
        compiler_params=pltpu.CompilerParams(collective_id=number, has_side_effects=True),
        name=name,
    )(*operands)


def on_device(
    density,
    leaf_target,
    geometry,
    near_list,
    far_list,
    node_list,
    basis_in,
    basis_out,
    transfer,
    node_points,
):
    leaves, nrhs_here, leaf_size = density.shape
    rank_size = basis_in.shape[1]
    nodes_here = transfer.shape[0]
    children = leaves // nodes_here
    wide = leaves + 2 * REACH
    first_leaf = lax.axis_index(("row", "col")) * leaves
    destination = leaf_target // leaves
    tree_slot = leaf_target % leaves
    count = lax.axis_size("row") * lax.axis_size("col")
    per = leaves // count
    ids = jnp.arange(leaves, dtype=jnp.int32)
    earlier = (destination[:, None] == destination) & (ids[:, None] > ids)
    rank = destination * per + jnp.sum(earlier.astype(jnp.int32), axis=1)
    placed = rank == ids[:, None]
    outgoing = density[jnp.sum(jnp.where(placed, ids, 0), axis=1)]
    out_slot = jnp.sum(jnp.where(placed, tree_slot, 0), axis=1).reshape(count, 1, per)
    bf16, f32 = jnp.bfloat16, jnp.float32
    arrived, arrived_slot, geo_wide = remote(
        exchange_kernel,
        "exchange",
        0,
        2 * count,
        (
            (density.shape, bf16),
            ((count, 1, leaf_size), jnp.int32),
            ((8, wide * leaf_size), f32),
        ),
        outgoing,
        jnp.pad(out_slot, ((0, 0), (0, 0), (0, leaf_size - per))),
        jnp.pad(geometry, ((0, 2), (0, 0))),
    )
    landed = arrived_slot[:, 0, :per].reshape(leaves)
    ordered = arrived[jnp.sum(jnp.where(landed == ids[:, None], ids, 0), axis=1)]
    skeleton = jnp.einsum(
        "tnl,trl->tnr", ordered, basis_in, preferred_element_type=jnp.float32
    ).astype(jnp.bfloat16)
    stacked = (
        skeleton.reshape(nodes_here, children, nrhs_here, rank_size)
        .transpose(0, 2, 1, 3)
        .reshape(nodes_here, nrhs_here, children * rank_size)
    )
    node_skel = jnp.einsum(
        "pnk,prk->pnr", stacked, transfer, preferred_element_type=jnp.float32
    ).astype(jnp.bfloat16)
    dens_wide, skel_wide, all_skel = remote(
        share_kernel,
        "share",
        1,
        count + 3,
        (
            ((wide + 1, nrhs_here, leaf_size), bf16),
            ((wide, nrhs_here, rank_size), bf16),
            ((nodes_here * count, nrhs_here, rank_size), bf16),
        ),
        ordered,
        skeleton,
        node_skel,
    )
    near = fill(compacted(near_list, REACH - first_leaf, wide))
    far = fill(compacted(far_list, REACH - first_leaf, wide))
    node = fill(compacted(node_list, wide + 1, wide))
    first_node = (first_leaf // children).reshape(1)
    node_pts = jnp.pad(node_points, ((0, 5), (0, 0)))
    return field(
        near, far, node, first_node, geo_wide, dens_wide, skel_wide, node_pts, all_skel,
        transfer, basis_out,
    )


def solution(mesh):
    return jax.shard_map(
        on_device,
        mesh=mesh,
        in_specs=(
            P(("grp", "row", "col"), None, None),
            P(("grp", "row", "col")),
            P(None, ("grp", "row", "col")),
            P(("grp", "row", "col"), None),
            P(("grp", "row", "col"), None),
            P(("grp", "row", "col"), None),
            P(("grp", "row", "col"), None, None),
            P(("grp", "row", "col"), None, None),
            P(("grp", "row", "col"), None, None),
            P(None, "grp"),
        ),
        out_specs=P(("grp", "row", "col"), None, None),
        check_vma=False,
    )
```
